32 devices in a mesh: section: 4 (over y, x), tok: 8 (over z, core).
Axes of the slice: x: 2, y: 2, z: 4, core: 2. Of those that a mesh axis runs over, the one named last changes fastest.
Arguments:
- activations: bfloat16 [8, 2048, 8192], P('section', 'tok'), may hold values from -12 to 12
- projection: bfloat16 [8192, 512], P('tok'), may hold values from -0.0625 to 0.0625
Outputs:
- sketch: float32 [8, 512, 512], P('section', None, 'tok')
- similarity: float32 [8, 2], P('section')
The draws below stay inside these ranges and needn't reach their ends.
All inputs are finite; a program needn't handle non-finite values.
Results may differ from the reference program's by a relative error of at most 0.0003.
Values may be sent and summed in bfloat16 or wider, within the bound.
A program may use at most 64 MiB of HBM per device.

```python
import jax
import jax.numpy as jnp
from jax import lax

D = 8192
RANK = 512
LAYERS = 8
TOKENS = 2048


def draw_activations(key, part):
    keyed = jax.random.fold_in(key, 11)
    key_base, key_weight, key_rows, key_mean, key_noise = jax.random.split(keyed, 5)
    shared = jax.random.normal(key_base, (TOKENS, D), jnp.float32)
    offset = jnp.zeros((D,), jnp.float32)
    mixing = jax.random.uniform(key_weight, (LAYERS,), jnp.float32, 0.2, 1.5)
    row_scale = jnp.exp(jax.random.uniform(key_rows, (LAYERS, TOKENS, 1), jnp.float32, jnp.log(0.3), jnp.log(3.0)))

    def one_layer(layer):
        noise = jax.random.normal(jax.random.fold_in(key_noise, layer), (TOKENS, D), jnp.float32)
        values = row_scale[layer] * (mixing[layer] * shared + noise) + offset
        return jnp.clip(values, -12.0, 12.0).astype(jnp.bfloat16)
    return lax.map(one_layer, jnp.arange(LAYERS, dtype=jnp.int32))


def block_levels(rng, shape, pieces, least, top_value):
    loudness, own = 1.0, jax.random.fold_in(rng, 6)
    for position, blocks in pieces:
        draws = jnp.exp(jax.random.uniform(jax.random.fold_in(own, position), (blocks,), jnp.float32, least / len(pieces), top_value / len(pieces)))
        loudness = loudness * jnp.repeat(draws, shape[position] // blocks).reshape([-1 if axis == position else 1 for axis in range(len(shape))])
    return loudness


def bell_draw(rng, shape, spread, most, cuts=(), held_as=jnp.bfloat16):
    level = block_levels(rng, shape, cuts, -0.22, 0.18) if cuts else 1.0
    drawn = jax.random.normal(rng, shape, jnp.float32) * spread * level
    return jnp.minimum(jnp.maximum(drawn, -most), most).astype(held_as)


def setup_inputs(seed: int = 0) -> dict:
    key_list = jax.random.split(jax.random.key(seed), 3)
    activations = draw_activations(jax.random.fold_in(key_list[2], 71), 0)
    projection = bell_draw(key_list[1], (D, RANK), D ** -0.5, 0.0625, ((0, 8),))
    return {"activations": activations, "projection": projection}


def reference(activations, projection):

    def layer_sketch(layer_acts):
        projected = jnp.dot(layer_acts, projection, preferred_element_type=jnp.float32)
        centred = projected - lax.optimization_barrier(jnp.sum(projected, axis=0)) / TOKENS
        return jnp.dot(centred.T, centred, precision=lax.Precision.HIGHEST)
    sketch = lax.map(layer_sketch, activations)
    flattened = sketch.reshape(sketch.shape[0], -1)
    squares = lax.optimization_barrier(jnp.sum(flattened * flattened, axis=1))
    before = jnp.concatenate([flattened[:1], flattened[:-1]], axis=0)
    beyond = jnp.concatenate([flattened[1:], flattened[-1:]], axis=0)
    square_before = jnp.concatenate([squares[:1], squares[:-1]])
    square_beyond = jnp.concatenate([squares[1:], squares[-1:]])
    earlier = lax.optimization_barrier(jnp.sum(flattened * before, axis=1)) / jnp.sqrt(squares * square_before)
    later = lax.optimization_barrier(jnp.sum(flattened * beyond, axis=1)) / jnp.sqrt(squares * square_beyond)
    return (sketch, jnp.stack([earlier, later], axis=1))
```

```python
import functools

import jax
import jax.numpy as jnp
from jax import lax
from jax.experimental import pallas as pl
from jax.experimental.pallas import tpu as pltpu
from jax.sharding import PartitionSpec as P

F32, BF16 = jnp.float32, jnp.bfloat16


def flip(index, mask, size):
    result, bit = 0, 1
    while bit < size:
        digit = (index // bit) % 2
        result = result + bit * ((1 - digit) if mask & bit else digit)
        bit *= 2
    return result


def snake(place, sections):
    half = sections // 2
    return jnp.where(place < half, place, 3 * half - 1 - place)


def kernel(
    sections, groups, layers, acts_hbm, proj_hbm, sketch_ref, sim_ref,
    acts, proj, total, left_op, right_op, gram, pair_in, line_in, mean_out, means, corr,
    edge_out, edge_in, prod_out, prods,
    acts_sem, own_sem, d2d_own, line_s, line_r, ring_s, ring_r, d2d_s, d2d_r,
    mean_s, mean_r, pair_s, pair_r, gl_s, gl_r, edge_s, edge_r, prod_s, prod_r,
):
    section = lax.axis_index("section")
    tok = lax.axis_index("tok")
    chips = groups // 2
    chip, core = tok // 2, tok % 2
    partner = chip * 2 + 1 - core
    rows = acts.shape[1]
    tok_rows = rows // layers
    depth = proj.shape[1]
    width = proj.shape[2]
    slab = width // groups
    half_ring = sections // 2
    piece = depth // sections
    part = piece // 2
    place = snake(section, sections)
    to_right = snake((place + 1) % sections, sections)
    to_left = snake((place + sections - 1) % sections, sections)

    own_copy = pltpu.make_async_copy(proj_hbm, proj.at[tok], own_sem)
    own_copy.start()
    order = [tok, partner]
    for k in range(1, chips):
        other = flip(chip, k, chips)
        order += [other * 2 + core, other * 2 + 1 - core]
    loads = []
    for n, t in enumerate(order):
        start = pl.multiple_of(t * depth, depth)
        loads.append(
            pltpu.make_async_copy(acts_hbm.at[:, pl.ds(start, depth)], acts.at[n], acts_sem.at[n])
        )
        loads[-1].start()

    barrier = pltpu.get_barrier_semaphore()
    for d in range(1, groups):
        pl.semaphore_signal(
            barrier, inc=1, device_id={"tok": (tok + d) % groups}, device_id_type=pl.DeviceIdType.MESH
        )
    for d in range(1, sections):
        pl.semaphore_signal(
            barrier, inc=1, device_id={"section": (section + d) % sections},
            device_id_type=pl.DeviceIdType.MESH,
        )
    pl.semaphore_wait(barrier, groups - 1 + sections - 1)

    pending = []

    def send(src, dst, send_sem, recv_sem, **where):
        copy = pltpu.make_async_remote_copy(
            src_ref=src, dst_ref=dst, send_sem=send_sem, recv_sem=recv_sem,
            device_id=where, device_id_type=pl.DeviceIdType.MESH,
        )
        copy.start()
        pending.append(copy)
        return copy

    def halves(t, at, h):
        start = pl.multiple_of((at % sections) * piece + h * part, part)
        return proj.at[t, pl.ds(start, part)]

    own_copy.wait()
    line = {}
    for k in range(1, chips):
        for h in range(2):
            ref = halves(tok, place, h)
            line[k, h] = send(
                ref, ref, line_s.at[k - 1, h], line_r.at[k - 1, h], tok=flip(chip, k, chips) * 2 + core
            )
    partner_slab = send(proj.at[tok], proj.at[tok], d2d_own.at[0], d2d_own.at[1], tok=partner)

    def multiply(n, first=False):
        loads[n].wait()
        product = jnp.dot(acts[n], proj[order[n]], preferred_element_type=F32)
        if first:
            total[...] = product
        else:
            total[...] += product

    multiply(0, True)
    partner_slab.wait_recv()
    multiply(1)

    shared = {k: [] for k in range(1, chips)}
    ring = {}

    def share(k, ref):
        n = len(shared[k])
        shared[k].append(send(ref, ref, d2d_s.at[k - 1, n], d2d_r.at[k - 1, n], tok=partner))

    def pass_on(k, j, way, h, ref):
        ring[k, j, way, h] = send(
            ref, ref, ring_s.at[k - 1, j - 1, way, h], ring_r.at[k - 1, j - 1, way, h],
            section=(to_right if way == 0 else to_left),
        )

    events = []
    for k in range(1, chips):
        events.append((2 * k, k, 0))
        for j in range(1, half_ring + 1):
            events.append((3 * k + j - 1, k, j))
    for _, k, j in sorted(events):
        t = order[2 * k]
        if j == 0:
            for h in range(2):
                line[k, h].wait_recv()
                ref = halves(t, place, h)
                for way in range(2):
                    if half_ring > 1 or way == h:
                        pass_on(k, 1, way, h, ref)
                share(k, ref)
        else:
            for h in range(2):
                for way in range(2):
                    if j == half_ring and way != h:
                        continue
                    ring[k, j, way, h].wait_recv()
                    at = place + sections - j if way == 0 else place + j
                    ref = halves(t, at, h)
                    if j < half_ring and (j + 1 < half_ring or way == h):
                        pass_on(k, j + 1, way, h, ref)
                    share(k, ref)
            if j == half_ring:
                multiply(2 * k)
                for copy in shared[k]:
                    copy.wait_recv()
                multiply(2 * k + 1)

    mean_out[...] = jnp.zeros_like(mean_out)
    for l in range(layers):
        block = total[l * tok_rows : (l + 1) * tok_rows]
        mean = jnp.sum(block, axis=0, keepdims=True) / tok_rows
        mean_out[l : l + 1] = mean
        block = block - mean
        high = block.astype(BF16)
        low = (block - high.astype(F32)).astype(BF16)
        left_op[l, :tok_rows] = high
        left_op[l, tok_rows : 2 * tok_rows] = high
        left_op[l, 2 * tok_rows :] = low
        right_op[l, :tok_rows] = high
        right_op[l, tok_rows : 2 * tok_rows] = low
        right_op[l, 2 * tok_rows :] = high
    mean_copies = []
    for k in range(1, groups):
        mean_copies.append(
            send(mean_out, means.at[k - 1], mean_s.at[k - 1], mean_r.at[k - 1], tok=flip(tok, k, groups))
        )

    pair = {}
    for l in range(layers):
        product = lax.dot_general(
            left_op[l], right_op[l], (((0,), (0,)), ((), ())), preferred_element_type=F32
        )
        for t in range(groups):
            gram[t, l] = product[t * slab : (t + 1) * slab]
        for k in list(range(1, chips)) + [0]:
            other = flip(chip, k, chips)
            pair[k, l] = send(
                gram.at[other * 2 + 1 - core, l], pair_in.at[k, l], pair_s.at[k, l], pair_r.at[k, l],
                tok=partner,
            )
    far = {}
    for l in range(layers):
        for k in list(range(1, chips)) + [0]:
            other = flip(chip, k, chips) * 2 + core
            pair[k, l].wait_recv()
            gram[other, l] = gram[other, l] + pair_in[k, l]
            if k:
                far[k, l] = send(
                    gram.at[other, l], line_in.at[k - 1, l], gl_s.at[k - 1, l], gl_r.at[k - 1, l],
                    tok=other,
                )

    for copy in mean_copies:
        copy.wait_recv()
    overall = mean_out[...]
    for k in range(1, groups):
        overall = overall + means[k - 1]
    overall = overall / groups
    for l in range(layers):
        shifts = [mean_out[l : l + 1] - overall[l : l + 1]]
        for k in range(1, groups):
            shifts.append(means[k - 1, l : l + 1] - overall[l : l + 1])
        shifts = jnp.concatenate(shifts, axis=0)
        outer = lax.dot_general(
            shifts, shifts * tok_rows, (((0,), (0,)), ((), ())),
            precision=lax.Precision.HIGHEST, preferred_element_type=F32,
        )
        for t in range(groups):
            corr[t, l] = outer[t * slab : (t + 1) * slab]

    edge = {}
    for l in range(layers):
        result = gram[tok, l] + corr[tok, l]
        for k in range(1, chips):
            far[k, l].wait_recv()
            result = result + line_in[k - 1, l]
        sketch_ref[l] = result
        if l == 0:
            edge_out[0] = result.astype(BF16)
            edge[0] = send(
                edge_out.at[0], edge_in.at[0], edge_s.at[0], edge_r.at[0],
                section=(section + sections - 1) % sections,
            )
        if l == layers - 1:
            edge_out[1] = result.astype(BF16)
            edge[1] = send(
                edge_out.at[1], edge_in.at[1], edge_s.at[1], edge_r.at[1],
                section=(section + 1) % sections,
            )

    def inner(first, second):
        columns = jnp.sum(first * second, axis=0, keepdims=True)
        lanes = columns[:, :128]
        for start in range(128, width, 128):
            lanes = lanes + columns[:, start : start + 128]
        return lanes

    prod_out[...] = jnp.zeros_like(prod_out)
    own = [sketch_ref[l] for l in range(layers)]
    for l in range(layers):
        prod_out[l : l + 1] = inner(own[l], own[l])
        if l:
            prod_out[layers + l - 1 : layers + l] = inner(own[l - 1], own[l])
    base = 2 * layers - 1
    edge[0].wait_recv()
    beyond = jnp.where(section == sections - 1, own[-1], edge_in[0].astype(F32))
    prod_out[base : base + 1] = inner(own[-1], beyond)
    prod_out[base + 1 : base + 2] = inner(beyond, beyond)
    edge[1].wait_recv()
    before = jnp.where(section == 0, own[0], edge_in[1].astype(F32))
    prod_out[base + 2 : base + 3] = inner(own[0], before)
    prod_out[base + 3 : base + 4] = inner(before, before)
    prod_copies = []
    for k in range(1, groups):
        prod_copies.append(
            send(prod_out, prods.at[k - 1], prod_s.at[k - 1], prod_r.at[k - 1], tok=flip(tok, k, groups))
        )
    products = prod_out[...]
    for k in range(1, groups):
        prod_copies[k - 1].wait_recv()
        products = products + prods[k - 1]
    products = jnp.broadcast_to(jnp.sum(products, axis=1, keepdims=True), products.shape)

    def item(i):
        return products[i : i + 1]

    squares = [item(base + 3)] + [item(l) for l in range(layers)] + [item(base + 1)]
    chained = [item(base + 2)] + [item(layers + l) for l in range(layers - 1)] + [item(base)]
    ratios = [chained[i] / jnp.sqrt(squares[i] * squares[i + 1]) for i in range(layers + 1)]
    sim_ref[...] = jnp.zeros_like(sim_ref)
    lane = lax.broadcasted_iota(jnp.int32, (1, 128), 1)
    for l in range(layers):
        sim_ref[l : l + 1] = jnp.where(lane == 0, ratios[l], ratios[l + 1])

    for copy in pending:
        copy.wait_send()


def local(sections, groups, activations, projection):
    layers, tok_rows, model_width = activations.shape
    depth, width = projection.shape
    rows = layers * tok_rows
    chips, slab = groups // 2, width // groups
    tall = -(-(2 * layers + 3) // 8) * 8
    dma = pltpu.SemaphoreType.DMA
    sketch, sim = pl.pallas_call(
        functools.partial(kernel, sections, groups, layers),
        out_shape=(
            jax.ShapeDtypeStruct((layers, slab, width), F32),
            jax.ShapeDtypeStruct((tall, 128), F32),
        ),
        in_specs=[pl.BlockSpec(memory_space=pl.ANY)] * 2,
        out_specs=(pl.BlockSpec(memory_space=pltpu.VMEM),) * 2,
        scratch_shapes=[
            pltpu.VMEM((groups, rows, depth), BF16),
            pltpu.VMEM((groups, depth, width), BF16),
            pltpu.VMEM((rows, width), F32),
            pltpu.VMEM((layers, 3 * tok_rows, width), BF16),
            pltpu.VMEM((layers, 3 * tok_rows, width), BF16),
            pltpu.VMEM((groups, layers, slab, width), F32),
            pltpu.VMEM((chips, layers, slab, width), F32),
            pltpu.VMEM((chips - 1, layers, slab, width), F32),
            pltpu.VMEM((tall, width), F32),
            pltpu.VMEM((groups - 1, tall, width), F32),
            pltpu.VMEM((groups, layers, slab, width), F32),
            pltpu.VMEM((2, slab, width), BF16),
            pltpu.VMEM((2, slab, width), BF16),
            pltpu.VMEM((tall, 128), F32),
            pltpu.VMEM((groups - 1, tall, 128), F32),
            dma((groups,)), dma(()), dma((2,)),
            dma((chips - 1, 2)), dma((chips - 1, 2)),
            dma((chips - 1, sections // 2, 2, 2)), dma((chips - 1, sections // 2, 2, 2)),
            dma((chips - 1, 2 * sections)), dma((chips - 1, 2 * sections)),
            dma((groups - 1,)), dma((groups - 1,)),
            dma((chips, layers)), dma((chips, layers)),
            dma((chips - 1, layers)), dma((chips - 1, layers)),
            dma((2,)), dma((2,)),
            dma((groups - 1,)), dma((groups - 1,)),
        ],
        compiler_params=pltpu.CompilerParams(
            collective_id=0, has_side_effects=True, vmem_limit_bytes=60 * 1024 * 1024
        ),
    )(activations.reshape(rows, model_width), projection)
    return jnp.swapaxes(sketch, 1, 2), sim[:layers, :2]


def solution(mesh):
    return jax.shard_map(
        functools.partial(local, mesh.shape["section"], mesh.shape["tok"]),
        mesh=mesh,
        in_specs=(P("section", "tok", None), P("tok", None)),
        out_specs=(P("section", None, "tok"), P("section", None)),
        check_vma=False,
    )
```

```python
import functools

import jax
import jax.numpy as jnp
from jax import lax
from jax.experimental import pallas as pl
from jax.experimental.pallas import tpu as pltpu
from jax.sharding import PartitionSpec as P

F32, BF16 = jnp.float32, jnp.bfloat16


def flip(index, mask, size):
    result, bit = 0, 1
    while bit < size:
        digit = (index // bit) % 2
        result = result + bit * ((1 - digit) if mask & bit else digit)
        bit *= 2
    return result


def nearest(chip, n, chips):
    short = jnp.minimum(chip, chips - 1 - chip)
    paired = n <= 2 * short
    distance = jnp.where(paired, (n + 1) // 2, n - short)
    lower = jnp.where(paired, n % 2 == 1, chip >= chips // 2)
    return jnp.where(lower, chip - distance, chip + distance)


def snake(place, sections):
    half = sections // 2
    return jnp.where(place < half, place, 3 * half - 1 - place)


def kernel(
    sections, groups, layers, acts_hbm, proj_hbm, sketch_ref, sim_ref,
    acts, proj, total, left_op, right_op, gram, pair_in, line_in, mean_out, means, corr,
    edge_out, edge_in, prod_out, prods, prev_prods,
    acts_sem, own_sem, d2d_own, line_s, line_r, ring_s, ring_r, d2d_s, d2d_r,
    mean_s, mean_r, pair_s, pair_r, gl_s, gl_r, edge_s, edge_r, prod_s, prod_r, prev_s, prev_r,
):
    section = lax.axis_index("section")
    tok = lax.axis_index("tok")
    chips = groups // 2
    chip, core = tok // 2, tok % 2
    partner = chip * 2 + 1 - core
    rows = acts.shape[1]
    tok_rows = rows // layers
    depth = proj.shape[1]
    width = proj.shape[2]
    slab = width // groups
    half_ring = sections // 2
    piece = depth // sections
    part = piece // 2
    place = snake(section, sections)
    to_right = snake((place + 1) % sections, sections)
    to_left = snake((place + sections - 1) % sections, sections)

    own_copy = pltpu.make_async_copy(proj_hbm, proj.at[tok], own_sem)
    own_copy.start()
    order = [tok, partner]
    for k in range(1, chips):
        other = nearest(chip, k, chips)
        order += [other * 2 + core, other * 2 + 1 - core]
    loads = []
    for n, t in enumerate(order):
        start = pl.multiple_of(t * depth, depth)
        loads.append(
            pltpu.make_async_copy(acts_hbm.at[:, pl.ds(start, depth)], acts.at[n], acts_sem.at[n])
        )
        loads[-1].start()

    barrier = pltpu.get_barrier_semaphore()
    for d in range(1, groups):
        pl.semaphore_signal(
            barrier, inc=1, device_id={"tok": (tok + d) % groups}, device_id_type=pl.DeviceIdType.MESH
        )
    for d in range(1, sections):
        pl.semaphore_signal(
            barrier, inc=1, device_id={"section": (section + d) % sections},
            device_id_type=pl.DeviceIdType.MESH,
        )
    beside = sorted({1, sections - 1})
    for away in beside:
        for d in range(1, groups):
            pl.semaphore_signal(
                barrier, inc=1,
                device_id={"section": (section + away) % sections, "tok": (tok + d) % groups},
                device_id_type=pl.DeviceIdType.MESH,
            )
    pl.semaphore_wait(barrier, (groups - 1) * (1 + len(beside)) + sections - 1)

    pending = []

    def send(src, dst, send_sem, recv_sem, **where):
        copy = pltpu.make_async_remote_copy(
            src_ref=src, dst_ref=dst, send_sem=send_sem, recv_sem=recv_sem,
            device_id=where, device_id_type=pl.DeviceIdType.MESH,
        )
        copy.start()
        pending.append(copy)
        return copy

    def halves(t, at, h):
        start = pl.multiple_of((at % sections) * piece + h * part, part)
        return proj.at[t, pl.ds(start, part)]

    own_copy.wait()

    def line_copy(source, h, step):
        ref = halves(source * 2 + core, place, h)
        return pltpu.make_async_remote_copy(
            src_ref=ref, dst_ref=ref,
            send_sem=line_s.at[source, h, (step + 1) // 2], recv_sem=line_r.at[source, h],
            device_id={"tok": (chip + step + chips) % chips * 2 + core},
            device_id_type=pl.DeviceIdType.MESH,
        )

    def along(source, h, action):
        for step in (-1, 1):
            inside = chip + step <= chips - 1 if step == 1 else chip + step >= 0
            away = source <= chip if step == 1 else source >= chip

            @pl.when(jnp.logical_and(inside, away))
            def _():
                action(line_copy(source, h, step))

    for h in range(2):
        along(chip, h, lambda copy: copy.start())
    partner_slab = send(proj.at[tok], proj.at[tok], d2d_own.at[0], d2d_own.at[1], tok=partner)

    def multiply(n, first=False):
        loads[n].wait()
        product = jnp.dot(acts[n], proj[order[n]], preferred_element_type=F32)
        if first:
            total[...] = product
        else:
            total[...] += product

    multiply(0, True)
    partner_slab.wait_recv()
    multiply(1)

    shared = {k: [] for k in range(1, chips)}
    ring = {}

    def share(k, ref):
        n = len(shared[k])
        shared[k].append(send(ref, ref, d2d_s.at[k - 1, n], d2d_r.at[k - 1, n], tok=partner))

    def pass_on(k, j, way, h, ref):
        ring[k, j, way, h] = send(
            ref, ref, ring_s.at[k - 1, j - 1, way, h], ring_r.at[k - 1, j - 1, way, h],
            section=(to_right if way == 0 else to_left),
        )

    events = []
    for k in range(1, chips):
        events.append((0.75 * k + 0.2, k, 0))
        for j in range(1, half_ring + 1):
            events.append((1.5 * k + 1.4 * j - 1.1, k, j))
        events.append((1.5 * k + 1.4 * half_ring - 0.9, k, half_ring + 1))
    for _, k, j in sorted(events):
        t = order[2 * k]
        if j == 0:
            for h in range(2):
                source = t // 2
                line_copy(source, h, 1).wait_recv()
                ref = halves(t, place, h)
                along(source, h, lambda copy: copy.start())
                for way in range(2):
                    if half_ring > 1 or way == h:
                        pass_on(k, 1, way, h, ref)
                share(k, ref)
        elif j <= half_ring:
            for h in range(2):
                for way in range(2):
                    if j == half_ring and way != h:
                        continue
                    ring[k, j, way, h].wait_recv()
                    at = place + sections - j if way == 0 else place + j
                    ref = halves(t, at, h)
                    if j < half_ring and (j + 1 < half_ring or way == h):
                        pass_on(k, j + 1, way, h, ref)
                    share(k, ref)
        else:
            multiply(2 * k)
            for copy in shared[k]:
                copy.wait_recv()
            multiply(2 * k + 1)

    mean_out[...] = jnp.zeros_like(mean_out)
    for l in range(layers):
        block = total[l * tok_rows : (l + 1) * tok_rows]
        mean = jnp.sum(block, axis=0, keepdims=True) / tok_rows
        mean_out[l : l + 1] = mean
        block = block - mean
        high = block.astype(BF16)
        low = (block - high.astype(F32)).astype(BF16)
        left_op[l, :tok_rows] = high
        left_op[l, tok_rows : 2 * tok_rows] = high
        left_op[l, 2 * tok_rows :] = low
        right_op[l, :tok_rows] = high
        right_op[l, tok_rows : 2 * tok_rows] = low
        right_op[l, 2 * tok_rows :] = high
    mean_copies = []
    for k in range(1, groups):
        mean_copies.append(
            send(mean_out, means.at[k - 1], mean_s.at[k - 1], mean_r.at[k - 1], tok=flip(tok, k, groups))
        )

    low_side = chip < chips // 2
    rank = jnp.where(low_side, chip, chips - 1 - chip)

    def mirror(d):
        return jnp.where(low_side, d, chips - 1 - d)

    pair = {}
    outward = [chips - 1 - d for d in range(chips)]
    for l in range(layers):
        product = lax.dot_general(
            left_op[l], right_op[l], (((0,), (0,)), ((), ())), preferred_element_type=F32
        )
        for t in range(groups):
            gram[t, l] = product[t * slab : (t + 1) * slab]
        for d in outward:
            pair[d, l] = send(
                gram.at[mirror(d) * 2 + 1 - core, l], pair_in.at[d, l], pair_s.at[d, l], pair_r.at[d, l],
                tok=partner,
            )

    def line_sum(d, l, primary):
        upward = low_side if primary else jnp.logical_not(low_side)
        way = jnp.where(upward, 0, 1)
        target = mirror(d)
        return pltpu.make_async_remote_copy(
            src_ref=gram.at[target * 2 + core, l], dst_ref=line_in.at[way, target, l],
            send_sem=gl_s.at[way, target, l], recv_sem=gl_r.at[way, target, l],
            device_id={"tok": jnp.clip(jnp.where(upward, chip + 1, chip - 1), 0, chips - 1) * 2 + core},
            device_id_type=pl.DeviceIdType.MESH,
        )

    def add_pair(d, l):
        pair[d, l].wait_recv()
        mine = mirror(d) * 2 + core
        gram[mine, l] = gram[mine, l] + pair_in[d, l]

    def arrive(d, l, primary):
        upward = low_side if primary else jnp.logical_not(low_side)
        way = jnp.where(upward, 0, 1)
        target = mirror(d)
        line_sum(d, l, primary).wait_recv()
        mine = target * 2 + core
        gram[mine, l] = gram[mine, l] + line_in[way, target, l]

    def arrive_own(l, primary):
        upward = low_side if primary else jnp.logical_not(low_side)
        way = jnp.where(upward, 0, 1)
        pltpu.make_async_remote_copy(
            src_ref=gram.at[tok, l], dst_ref=line_in.at[way, chip, l],
            send_sem=gl_s.at[way, chip, l], recv_sem=gl_r.at[way, chip, l],
            device_id={"tok": partner}, device_id_type=pl.DeviceIdType.MESH,
        ).wait_recv()
        gram[tok, l] = gram[tok, l] + line_in[way, chip, l]

    def forward(d, l, primary):
        @pl.when(d > rank if primary else d < rank)
        def _():
            if primary:
                @pl.when(rank > 0)
                def _():
                    arrive(d, l, primary)
            else:
                arrive(d, l, primary)
            line_sum(d, l, primary).start()

    def correct():
        for copy in mean_copies:
            copy.wait_recv()
        overall = mean_out[...]
        for k in range(1, groups):
            overall = overall + means[k - 1]
        overall = overall / groups
        for l in range(layers):
            shifts = [mean_out[l : l + 1] - overall[l : l + 1]]
            for k in range(1, groups):
                shifts.append(means[k - 1, l : l + 1] - overall[l : l + 1])
            shifts = jnp.concatenate(shifts, axis=0)
            outer = lax.dot_general(
                shifts, shifts * tok_rows, (((0,), (0,)), ((), ())),
                precision=lax.Precision.HIGHEST, preferred_element_type=F32,
            )
            for t in range(groups):
                corr[t, l] = outer[t * slab : (t + 1) * slab]

    steps = []
    for d in range(chips):
        for l in range(layers):
            turn = (chips - 1 - d) * layers + l
            steps.append((turn, 1, d, l))
            if d < chips - 1:
                steps.append((d * layers + l + layers - 0.5, 0, d, l))
    early = True
    for turn, primary, d, l in sorted(steps):
        if turn > layers - 1 and early:
            early = False
            for other in outward[1:]:
                for m in range(layers):
                    add_pair(other, m)
            correct()
        if early:
            add_pair(d, l)
        if d > 0 or not primary:
            forward(d, l, bool(primary))

    edge = None
    for l in range(layers):
        @pl.when(rank > 0)
        def _():
            arrive_own(l, True)

        arrive_own(l, False)
        result = gram[tok, l] + corr[tok, l]
        sketch_ref[l] = result
        if l == 0:
            edge_out[...] = result.astype(BF16)
            edge = send(
                edge_out, edge_in, edge_s, edge_r, section=(section + sections - 1) % sections
            )

    def inner(first, second):
        columns = jnp.sum(first * second, axis=0, keepdims=True)
        lanes = columns[:, :128]
        for start in range(128, width, 128):
            lanes = lanes + columns[:, start : start + 128]
        return lanes

    prod_out[...] = jnp.zeros_like(prod_out)
    own = [sketch_ref[l] for l in range(layers)]
    for l in range(layers):
        prod_out[l : l + 1] = inner(own[l], own[l])
        if l:
            prod_out[layers + l - 1 : layers + l] = inner(own[l - 1], own[l])
    base = 2 * layers - 1
    edge.wait_recv()
    beyond = edge_in[...].astype(F32)
    prod_out[base : base + 1] = inner(own[-1], beyond)
    prod_out[base + 1 : base + 2] = inner(beyond, beyond)
    prod_copies, prev_copies = [], []
    for k in range(groups):
        other = flip(tok, k, groups)
        prev_copies.append(
            send(prod_out, prev_prods.at[k], prev_s.at[k], prev_r.at[k],
                 section=(section + 1) % sections, tok=other)
        )
        if k:
            prod_copies.append(
                send(prod_out, prods.at[k - 1], prod_s.at[k - 1], prod_r.at[k - 1], tok=other)
            )
    products = prod_out[...]
    for k in range(1, groups):
        prod_copies[k - 1].wait_recv()
        products = products + prods[k - 1]
    prev_copies[0].wait_recv()
    earlier = prev_prods[0]
    for k in range(1, groups):
        prev_copies[k].wait_recv()
        earlier = earlier + prev_prods[k]
    products = jnp.broadcast_to(jnp.sum(products, axis=1, keepdims=True), products.shape)
    earlier = jnp.broadcast_to(jnp.sum(earlier, axis=1, keepdims=True), earlier.shape)

    def item(i):
        return products[i : i + 1]

    first, last = section == 0, section == sections - 1
    before = jnp.where(first, item(0), earlier[layers - 1 : layers])
    before_cross = jnp.where(first, item(0), earlier[base : base + 1])
    beyond_square = jnp.where(last, item(layers - 1), item(base + 1))
    beyond_cross = jnp.where(last, item(layers - 1), item(base))
    squares = [before] + [item(l) for l in range(layers)] + [beyond_square]
    chained = [before_cross] + [item(layers + l) for l in range(layers - 1)] + [beyond_cross]
    ratios = [chained[i] / jnp.sqrt(squares[i] * squares[i + 1]) for i in range(layers + 1)]
    sim_ref[...] = jnp.zeros_like(sim_ref)
    lane = lax.broadcasted_iota(jnp.int32, (1, 128), 1)
    for l in range(layers):
        sim_ref[l : l + 1] = jnp.where(lane == 0, ratios[l], ratios[l + 1])

    for copy in pending:
        copy.wait_send()
    for d in range(chips):
        for l in range(layers):
            for primary in (True, False):
                @pl.when(d > rank if primary else d < rank)
                def _():
                    line_sum(d, l, primary).wait_send()
    for source in [chip] + [t // 2 for t in order[2::2]]:
        for h in range(2):
            along(source, h, lambda copy: copy.wait_send())


def local(sections, groups, activations, projection):
    layers, tok_rows, model_width = activations.shape
    depth, width = projection.shape
    rows = layers * tok_rows
    chips, slab = groups // 2, width // groups
    tall = -(-(2 * layers + 3) // 8) * 8
    dma = pltpu.SemaphoreType.DMA
    sketch, sim = pl.pallas_call(
        functools.partial(kernel, sections, groups, layers),
        out_shape=(
            jax.ShapeDtypeStruct((layers, slab, width), F32),
            jax.ShapeDtypeStruct((tall, 128), F32),
        ),
        in_specs=[pl.BlockSpec(memory_space=pl.ANY)] * 2,
        out_specs=(pl.BlockSpec(memory_space=pltpu.VMEM),) * 2,
        scratch_shapes=[
            pltpu.VMEM((groups, rows, depth), BF16),
            pltpu.VMEM((groups, depth, width), BF16),
            pltpu.VMEM((rows, width), F32),
            pltpu.VMEM((layers, 3 * tok_rows, width), BF16),
            pltpu.VMEM((layers, 3 * tok_rows, width), BF16),
            pltpu.VMEM((groups, layers, slab, width), F32),
            pltpu.VMEM((chips, layers, slab, width), F32),
            pltpu.VMEM((2, chips, layers, slab, width), F32),
            pltpu.VMEM((tall, width), F32),
            pltpu.VMEM((groups - 1, tall, width), F32),
            pltpu.VMEM((groups, layers, slab, width), F32),
            pltpu.VMEM((slab, width), BF16),
            pltpu.VMEM((slab, width), BF16),
            pltpu.VMEM((tall, 128), F32),
            pltpu.VMEM((groups - 1, tall, 128), F32),
            pltpu.VMEM((groups, tall, 128), F32),
            dma((groups,)), dma(()), dma((2,)),
            dma((chips, 2, 2)), dma((chips, 2)),
            dma((chips - 1, sections // 2, 2, 2)), dma((chips - 1, sections // 2, 2, 2)),
            dma((chips - 1, 2 * sections)), dma((chips - 1, 2 * sections)),
            dma((groups - 1,)), dma((groups - 1,)),
            dma((chips, layers)), dma((chips, layers)),
            dma((2, chips, layers)), dma((2, chips, layers)),
            dma(()), dma(()),
            dma((groups - 1,)), dma((groups - 1,)),
            dma((groups,)), dma((groups,)),
        ],
        compiler_params=pltpu.CompilerParams(
            collective_id=0, has_side_effects=True, vmem_limit_bytes=60 * 1024 * 1024
        ),
    )(activations.reshape(rows, model_width), projection)
    return jnp.swapaxes(sketch, 1, 2), sim[:layers, :2]


def solution(mesh):
    return jax.shard_map(
        functools.partial(local, mesh.shape["section"], mesh.shape["tok"]),
        mesh=mesh,
        in_specs=(P("section", "tok", None), P("tok", None)),
        out_specs=(P("section", None, "tok"), P("section", None)),
        check_vma=False,
    )
```

```python
import functools

import jax
import jax.numpy as jnp
from jax import lax
from jax.experimental import pallas as pl
from jax.experimental.pallas import tpu as pltpu
from jax.sharding import PartitionSpec as P

F32, BF16 = jnp.float32, jnp.bfloat16


def flip(index, mask, size):
    result, bit = 0, 1
    while bit < size:
        digit = (index // bit) % 2
        result = result + bit * ((1 - digit) if mask & bit else digit)
        bit *= 2
    return result


def nearest(chip, n, chips):
    short = jnp.minimum(chip, chips - 1 - chip)
    paired = n <= 2 * short
    distance = jnp.where(paired, (n + 1) // 2, n - short)
    lower = jnp.where(paired, n % 2 == 1, chip >= chips // 2)
    return jnp.where(lower, chip - distance, chip + distance)


def snake(place, sections):
    half = sections // 2
    return jnp.where(place < half, place, 3 * half - 1 - place)


def kernel(
    sections, groups, layers, acts_hbm, proj_hbm, sketch_ref, sim_ref,
    acts, proj, total, left_op, right_op, gram, pair_in, line_in, mean_out, means, corr,
    edge_out, edge_in, prod_out, prods, prev_prods,
    acts_sem, own_sem, d2d_own, line_s, line_r, ring_s, ring_r, d2d_s, d2d_r,
    mean_s, mean_r, pair_s, pair_r, gl_s, gl_r, edge_s, edge_r, prod_s, prod_r, prev_s, prev_r,
):
    section = lax.axis_index("section")
    tok = lax.axis_index("tok")
    chips = groups // 2
    chip, core = tok // 2, tok % 2
    partner = chip * 2 + 1 - core
    rows = acts.shape[1]
    tok_rows = rows // layers
    depth = proj.shape[1]
    width = proj.shape[2]
    slab = width // groups
    half_ring = sections // 2
    piece = depth // sections
    part = piece // 2
    cut = part // 2 if part % 32 == 0 else 0
    place = snake(section, sections)
    to_right = snake((place + 1) % sections, sections)
    to_left = snake((place + sections - 1) % sections, sections)

    own_copy = pltpu.make_async_copy(proj_hbm, proj.at[tok], own_sem)
    own_copy.start()
    order = [tok, partner]
    for k in range(1, chips):
        other = nearest(chip, k, chips)
        order += [other * 2 + core, other * 2 + 1 - core]
    loads = []
    for n, t in enumerate(order):
        start = pl.multiple_of(t * depth, depth)
        loads.append(
            pltpu.make_async_copy(acts_hbm.at[:, pl.ds(start, depth)], acts.at[n], acts_sem.at[n])
        )
        loads[-1].start()

    barrier = pltpu.get_barrier_semaphore()
    for d in range(1, groups):
        pl.semaphore_signal(
            barrier, inc=1, device_id={"tok": (tok + d) % groups}, device_id_type=pl.DeviceIdType.MESH
        )
    for d in range(1, sections):
        pl.semaphore_signal(
            barrier, inc=1, device_id={"section": (section + d) % sections},
            device_id_type=pl.DeviceIdType.MESH,
        )
    beside = sorted({1, sections - 1})
    for away in beside:
        for d in range(1, groups):
            pl.semaphore_signal(
                barrier, inc=1,
                device_id={"section": (section + away) % sections, "tok": (tok + d) % groups},
                device_id_type=pl.DeviceIdType.MESH,
            )
    pl.semaphore_wait(barrier, (groups - 1) * (1 + len(beside)) + sections - 1)

    pending = []

    def send(src, dst, send_sem, recv_sem, **where):
        copy = pltpu.make_async_remote_copy(
            src_ref=src, dst_ref=dst, send_sem=send_sem, recv_sem=recv_sem,
            device_id=where, device_id_type=pl.DeviceIdType.MESH,
        )
        copy.start()
        pending.append(copy)
        return copy

    def halves(t, at, h, last=False):
        start, size = (at % sections) * piece + h * part, part
        if last:
            start, size = start + h * cut, part - cut
        align = cut if cut else part
        return proj.at[t, pl.ds(pl.multiple_of(start, align), size)]

    def line_ref(t, h):
        if h < 2:
            return halves(t, place, h)
        start = (place + half_ring) % sections * piece + part - cut
        return proj.at[t, pl.ds(pl.multiple_of(start, cut), 2 * cut)]

    own_copy.wait()

    def line_copy(source, h, step):
        ref = line_ref(source * 2 + core, h)
        return pltpu.make_async_remote_copy(
            src_ref=ref, dst_ref=ref,
            send_sem=line_s.at[source, h, (step + 1) // 2], recv_sem=line_r.at[source, h],
            device_id={"tok": (chip + step + chips) % chips * 2 + core},
            device_id_type=pl.DeviceIdType.MESH,
        )

    def along(source, h, action):
        for step in (-1, 1):
            inside = chip + step <= chips - 1 if step == 1 else chip + step >= 0
            away = source <= chip if step == 1 else source >= chip

            @pl.when(jnp.logical_and(inside, away))
            def _():
                action(line_copy(source, h, step))

    for h in range(2):
        along(chip, h, lambda copy: copy.start())
    outer_chip = jnp.minimum(chip, chips - 1 - chip) == 0
    if cut:
        @pl.when(outer_chip)
        def _():
            along(chip, 2, lambda copy: copy.start())
    partner_slab = send(proj.at[tok], proj.at[tok], d2d_own.at[0], d2d_own.at[1], tok=partner)

    def multiply(n, first=False):
        loads[n].wait()
        product = jnp.dot(acts[n], proj[order[n]], preferred_element_type=F32)
        if first:
            total[...] = product
        else:
            total[...] += product

    multiply(0, True)
    partner_slab.wait_recv()
    multiply(1)

    shared = {k: [] for k in range(1, chips)}
    ring = {}

    def share(k, ref):
        n = len(shared[k])
        shared[k].append(send(ref, ref, d2d_s.at[k - 1, n], d2d_r.at[k - 1, n], tok=partner))

    def pass_on(k, j, way, h, ref):
        ring[k, j, way, h] = send(
            ref, ref, ring_s.at[k - 1, j - 1, way, h], ring_r.at[k - 1, j - 1, way, h],
            section=(to_right if way == 0 else to_left),
        )

    events = []
    for k in range(1, chips):
        events.append((0.75 * k + 0.2, k, 0))
        for j in range(1, half_ring + 1):
            events.append((1.5 * k + 1.4 * j - 1.1, k, j))
        if cut:
            events.append((0.75 * chips - 0.5 if k == 1 else 3.3 + 0.02 * k, k, -1))
        events.append((1.5 * k + 1.4 * half_ring - 0.9, k, half_ring + 1))
    for _, k, j in sorted(events):
        t = order[2 * k]
        source = t // 2
        if j < 0:
            line_copy(source, 2, 1).wait_recv()
            along(source, 2, lambda copy: copy.start())
            share(k, line_ref(t, 2))
        elif j == 0:
            for h in range(2):
                line_copy(source, h, 1).wait_recv()
                ref = halves(t, place, h)
                along(source, h, lambda copy: copy.start())
                for way in range(2):
                    if half_ring > 1 or way == h:
                        pass_on(k, 1, way, h, halves(t, place, h, half_ring == 1))
                share(k, ref)
            if k == min(2, chips - 1) and cut:
                @pl.when(jnp.logical_not(outer_chip))
                def _():
                    along(chip, 2, lambda copy: copy.start())
        elif j <= half_ring:
            for h in range(2):
                for way in range(2):
                    if j == half_ring and way != h:
                        continue
                    ring[k, j, way, h].wait_recv()
                    at = place + sections - j if way == 0 else place + j
                    if j < half_ring and (j + 1 < half_ring or way == h):
                        pass_on(k, j + 1, way, h, halves(t, at, h, j + 1 == half_ring))
                    share(k, halves(t, at, h, j == half_ring))
        else:
            multiply(2 * k)
            for copy in shared[k]:
                copy.wait_recv()
            multiply(2 * k + 1)

    mean_out[...] = jnp.zeros_like(mean_out)
    for l in range(layers):
        block = total[l * tok_rows : (l + 1) * tok_rows]
        mean = jnp.sum(block, axis=0, keepdims=True) / tok_rows
        mean_out[l : l + 1] = mean
        block = block - mean
        high = block.astype(BF16)
        low = (block - high.astype(F32)).astype(BF16)
        left_op[l, :tok_rows] = high
        left_op[l, tok_rows : 2 * tok_rows] = high
        left_op[l, 2 * tok_rows :] = low
        right_op[l, :tok_rows] = high
        right_op[l, tok_rows : 2 * tok_rows] = low
        right_op[l, 2 * tok_rows :] = high
    mean_copies = []
    for k in range(1, groups):
        mean_copies.append(
            send(mean_out, means.at[k - 1], mean_s.at[k - 1], mean_r.at[k - 1], tok=flip(tok, k, groups))
        )

    low_side = chip < chips // 2
    rank = jnp.where(low_side, chip, chips - 1 - chip)

    def mirror(d):
        return jnp.where(low_side, d, chips - 1 - d)

    pair = {}
    outward = [chips - 1 - d for d in range(chips)]
    for l in range(layers):
        product = lax.dot_general(
            left_op[l], right_op[l], (((0,), (0,)), ((), ())), preferred_element_type=F32
        )
        for t in range(groups):
            gram[t, l] = product[t * slab : (t + 1) * slab]
        for d in outward:
            pair[d, l] = send(
                gram.at[mirror(d) * 2 + 1 - core, l], pair_in.at[d, l], pair_s.at[d, l], pair_r.at[d, l],
                tok=partner,
            )

    def line_sum(d, l, primary):
        upward = low_side if primary else jnp.logical_not(low_side)
        way = jnp.where(upward, 0, 1)
        target = mirror(d)
        return pltpu.make_async_remote_copy(
            src_ref=gram.at[target * 2 + core, l], dst_ref=line_in.at[way, target, l],
            send_sem=gl_s.at[way, target, l], recv_sem=gl_r.at[way, target, l],
            device_id={"tok": jnp.clip(jnp.where(upward, chip + 1, chip - 1), 0, chips - 1) * 2 + core},
            device_id_type=pl.DeviceIdType.MESH,
        )

    def add_pair(d, l):
        pair[d, l].wait_recv()
        mine = mirror(d) * 2 + core
        gram[mine, l] = gram[mine, l] + pair_in[d, l]

    def arrive(d, l, primary):
        upward = low_side if primary else jnp.logical_not(low_side)
        way = jnp.where(upward, 0, 1)
        target = mirror(d)
        line_sum(d, l, primary).wait_recv()
        mine = target * 2 + core
        gram[mine, l] = gram[mine, l] + line_in[way, target, l]

    def arrive_own(l, primary):
        upward = low_side if primary else jnp.logical_not(low_side)
        way = jnp.where(upward, 0, 1)
        pltpu.make_async_remote_copy(
            src_ref=gram.at[tok, l], dst_ref=line_in.at[way, chip, l],
            send_sem=gl_s.at[way, chip, l], recv_sem=gl_r.at[way, chip, l],
            device_id={"tok": partner}, device_id_type=pl.DeviceIdType.MESH,
        ).wait_recv()
        gram[tok, l] = gram[tok, l] + line_in[way, chip, l]

    def forward(d, l, primary):
        @pl.when(d > rank if primary else d < rank)
        def _():
            if primary:
                @pl.when(rank > 0)
                def _():
                    arrive(d, l, primary)
            else:
                arrive(d, l, primary)
            line_sum(d, l, primary).start()

    def correct():
        for copy in mean_copies:
            copy.wait_recv()
        overall = mean_out[...]
        for k in range(1, groups):
            overall = overall + means[k - 1]
        overall = overall / groups
        for l in range(layers):
            shifts = [mean_out[l : l + 1] - overall[l : l + 1]]
            for k in range(1, groups):
                shifts.append(means[k - 1, l : l + 1] - overall[l : l + 1])
            shifts = jnp.concatenate(shifts, axis=0)
            outer = lax.dot_general(
                shifts, shifts * tok_rows, (((0,), (0,)), ((), ())),
                precision=lax.Precision.HIGHEST, preferred_element_type=F32,
            )
            for t in range(groups):
                corr[t, l] = outer[t * slab : (t + 1) * slab]

    steps = []
    for d in range(chips):
        for l in range(layers):
            turn = (chips - 1 - d) * layers + l
            steps.append((turn, 1, d, l))
            if d < chips - 1:
                steps.append((d * layers + l + layers - 0.5, 0, d, l))
    early = True
    for turn, primary, d, l in sorted(steps):
        if turn > layers - 1 and early:
            early = False
            for other in outward[1:]:
                for m in range(layers):
                    add_pair(other, m)
            correct()
        if early:
            add_pair(d, l)
        if d > 0 or not primary:
            forward(d, l, bool(primary))

    edge = None
    for l in range(layers):
        @pl.when(rank > 0)
        def _():
            arrive_own(l, True)

        arrive_own(l, False)
        result = gram[tok, l] + corr[tok, l]
        sketch_ref[l] = result
        if l == 0:
            edge_out[...] = result.astype(BF16)
            edge = send(
                edge_out, edge_in, edge_s, edge_r, section=(section + sections - 1) % sections
            )

    def inner(first, second):
        columns = jnp.sum(first * second, axis=0, keepdims=True)
        lanes = columns[:, :128]
        for start in range(128, width, 128):
            lanes = lanes + columns[:, start : start + 128]
        return lanes

    prod_out[...] = jnp.zeros_like(prod_out)
    own = [sketch_ref[l] for l in range(layers)]
    for l in range(layers):
        prod_out[l : l + 1] = inner(own[l], own[l])
        if l:
            prod_out[layers + l - 1 : layers + l] = inner(own[l - 1], own[l])
    base = 2 * layers - 1
    edge.wait_recv()
    beyond = edge_in[...].astype(F32)
    prod_out[base : base + 1] = inner(own[-1], beyond)
    prod_out[base + 1 : base + 2] = inner(beyond, beyond)
    prod_copies, prev_copies = [], []
    for k in range(groups):
        other = flip(tok, k, groups)
        prev_copies.append(
            send(prod_out, prev_prods.at[k], prev_s.at[k], prev_r.at[k],
                 section=(section + 1) % sections, tok=other)
        )
        if k:
            prod_copies.append(
                send(prod_out, prods.at[k - 1], prod_s.at[k - 1], prod_r.at[k - 1], tok=other)
            )
    products = prod_out[...]
    for k in range(1, groups):
        prod_copies[k - 1].wait_recv()
        products = products + prods[k - 1]
    prev_copies[0].wait_recv()
    earlier = prev_prods[0]
    for k in range(1, groups):
        prev_copies[k].wait_recv()
        earlier = earlier + prev_prods[k]
    products = jnp.broadcast_to(jnp.sum(products, axis=1, keepdims=True), products.shape)
    earlier = jnp.broadcast_to(jnp.sum(earlier, axis=1, keepdims=True), earlier.shape)

    def item(i):
        return products[i : i + 1]

    first, last = section == 0, section == sections - 1
    before = jnp.where(first, item(0), earlier[layers - 1 : layers])
    before_cross = jnp.where(first, item(0), earlier[base : base + 1])
    beyond_square = jnp.where(last, item(layers - 1), item(base + 1))
    beyond_cross = jnp.where(last, item(layers - 1), item(base))
    squares = [before] + [item(l) for l in range(layers)] + [beyond_square]
    chained = [before_cross] + [item(layers + l) for l in range(layers - 1)] + [beyond_cross]
    ratios = [chained[i] / jnp.sqrt(squares[i] * squares[i + 1]) for i in range(layers + 1)]
    sim_ref[...] = jnp.zeros_like(sim_ref)
    lane = lax.broadcasted_iota(jnp.int32, (1, 128), 1)
    for l in range(layers):
        sim_ref[l : l + 1] = jnp.where(lane == 0, ratios[l], ratios[l + 1])

    for copy in pending:
        copy.wait_send()
    for d in range(chips):
        for l in range(layers):
            for primary in (True, False):
                @pl.when(d > rank if primary else d < rank)
                def _():
                    line_sum(d, l, primary).wait_send()
    for source in [chip] + [t // 2 for t in order[2::2]]:
        for h in range(3 if cut else 2):
            along(source, h, lambda copy: copy.wait_send())


def finish(sketch_in, sim_in, sketch_out, sim_out):
    sketch_out[...] = sketch_in[...]
    sim_out[...] = sim_in[: sim_out.shape[0], : sim_out.shape[1]]


def local(sections, groups, activations, projection):
    layers, tok_rows, model_width = activations.shape
    depth, width = projection.shape
    rows = layers * tok_rows
    chips, slab = groups // 2, width // groups
    tall = -(-(2 * layers + 3) // 8) * 8
    dma = pltpu.SemaphoreType.DMA
    sketch, sim = pl.pallas_call(
        functools.partial(kernel, sections, groups, layers),
        out_shape=(
            jax.ShapeDtypeStruct((layers, slab, width), F32),
            jax.ShapeDtypeStruct((tall, 128), F32),
        ),
        in_specs=[pl.BlockSpec(memory_space=pl.ANY)] * 2,
        out_specs=(pl.BlockSpec(memory_space=pltpu.VMEM),) * 2,
        scratch_shapes=[
            pltpu.VMEM((groups, rows, depth), BF16),
            pltpu.VMEM((groups, depth, width), BF16),
            pltpu.VMEM((rows, width), F32),
            pltpu.VMEM((layers, 3 * tok_rows, width), BF16),
            pltpu.VMEM((layers, 3 * tok_rows, width), BF16),
            pltpu.VMEM((groups, layers, slab, width), F32),
            pltpu.VMEM((chips, layers, slab, width), F32),
            pltpu.VMEM((2, chips, layers, slab, width), F32),
            pltpu.VMEM((tall, width), F32),
            pltpu.VMEM((groups - 1, tall, width), F32),
            pltpu.VMEM((groups, layers, slab, width), F32),
            pltpu.VMEM((slab, width), BF16),
            pltpu.VMEM((slab, width), BF16),
            pltpu.VMEM((tall, 128), F32),
            pltpu.VMEM((groups - 1, tall, 128), F32),
            pltpu.VMEM((groups, tall, 128), F32),
            dma((groups,)), dma(()), dma((2,)),
            dma((chips, 3, 2)), dma((chips, 3)),
            dma((chips - 1, sections // 2, 2, 2)), dma((chips - 1, sections // 2, 2, 2)),
            dma((chips - 1, 2 * sections + 1)), dma((chips - 1, 2 * sections + 1)),
            dma((groups - 1,)), dma((groups - 1,)),
            dma((chips, layers)), dma((chips, layers)),
            dma((2, chips, layers)), dma((2, chips, layers)),
            dma(()), dma(()),
            dma((groups - 1,)), dma((groups - 1,)),
            dma((groups,)), dma((groups,)),
        ],
        compiler_params=pltpu.CompilerParams(
            collective_id=0, has_side_effects=True, vmem_limit_bytes=60 * 1024 * 1024
        ),
    )(activations.reshape(rows, model_width), projection)
    sketch, similarity = pl.pallas_call(
        finish,
        out_shape=(
            jax.ShapeDtypeStruct((layers, slab, width), F32),
            jax.ShapeDtypeStruct((layers, 2), F32),
        ),
        in_specs=[pl.BlockSpec(memory_space=pltpu.VMEM)] * 2,
        out_specs=(pl.BlockSpec(memory_space=pltpu.VMEM),) * 2,
    )(sketch, sim)
    return jnp.swapaxes(sketch, 1, 2), similarity


def solution(mesh):
    return jax.shard_map(
        functools.partial(local, mesh.shape["section"], mesh.shape["tok"]),
        mesh=mesh,
        in_specs=(P("section", "tok", None), P("tok", None)),
        out_specs=(P("section", None, "tok"), P("section", None)),
        check_vma=False,
    )
```

```python
import functools

import jax
import jax.numpy as jnp
from jax import lax
from jax.experimental import pallas as pl
from jax.experimental.pallas import tpu as pltpu
from jax.sharding import PartitionSpec as P

F32, BF16 = jnp.float32, jnp.bfloat16


def flip(index, mask, size):
    result, bit = 0, 1
    while bit < size:
        digit = (index // bit) % 2
        result = result + bit * ((1 - digit) if mask & bit else digit)
        bit *= 2
    return result


def nearest(chip, n, chips):
    short = jnp.minimum(chip, chips - 1 - chip)
    paired = n <= 2 * short
    distance = jnp.where(paired, (n + 1) // 2, n - short)
    lower = jnp.where(paired, n % 2 == 1, chip >= chips // 2)
    return jnp.where(lower, chip - distance, chip + distance)


def snake(place, sections):
    half = sections // 2
    return jnp.where(place < half, place, 3 * half - 1 - place)


def kernel(
    sections, groups, layers, acts_hbm, proj_hbm, sketch_ref, sim_ref,
    acts, proj, total, left_op, right_op, gram, pair_in, line_in, mean_out, means, corr,
    edge_out, edge_in, prod_out, prods, prev_prods,
    acts_sem, own_sem, d2d_own, line_s, line_r, ring_s, ring_r, d2d_s, d2d_r,
    mean_s, mean_r, pair_s, pair_r, gl_s, gl_r, edge_s, edge_r, prod_s, prod_r, prev_s, prev_r,
):
    section = lax.axis_index("section")
    tok = lax.axis_index("tok")
    chips = groups // 2
    chip, core = tok // 2, tok % 2
    partner = chip * 2 + 1 - core
    rows = acts.shape[1]
    tok_rows = rows // layers
    depth = proj.shape[1]
    width = proj.shape[2]
    slab = width // groups
    half_ring = sections // 2
    piece = depth // sections
    part = piece // 2
    cut = part // 2 if part % 32 == 0 else 0
    place = snake(section, sections)
    to_right = snake((place + 1) % sections, sections)
    to_left = snake((place + sections - 1) % sections, sections)

    own_copy = pltpu.make_async_copy(proj_hbm, proj.at[tok], own_sem)
    own_copy.start()
    order = [tok, partner]
    for k in range(1, chips):
        other = nearest(chip, k, chips)
        order += [other * 2 + core, other * 2 + 1 - core]
    loads = []
    for n, t in enumerate(order):
        start = pl.multiple_of(t * depth, depth)
        loads.append(
            pltpu.make_async_copy(acts_hbm.at[:, pl.ds(start, depth)], acts.at[n], acts_sem.at[n])
        )
        loads[-1].start()

    barrier = pltpu.get_barrier_semaphore()
    for d in range(1, groups):
        pl.semaphore_signal(
            barrier, inc=1, device_id={"tok": (tok + d) % groups}, device_id_type=pl.DeviceIdType.MESH
        )
    for d in range(1, sections):
        pl.semaphore_signal(
            barrier, inc=1, device_id={"section": (section + d) % sections},
            device_id_type=pl.DeviceIdType.MESH,
        )
    beside = sorted({1, sections - 1})
    for away in beside:
        for d in range(1, groups):
            pl.semaphore_signal(
                barrier, inc=1,
                device_id={"section": (section + away) % sections, "tok": (tok + d) % groups},
                device_id_type=pl.DeviceIdType.MESH,
            )
    pl.semaphore_wait(barrier, (groups - 1) * (1 + len(beside)) + sections - 1)

    pending = []

    def send(src, dst, send_sem, recv_sem, **where):
        copy = pltpu.make_async_remote_copy(
            src_ref=src, dst_ref=dst, send_sem=send_sem, recv_sem=recv_sem,
            device_id=where, device_id_type=pl.DeviceIdType.MESH,
        )
        copy.start()
        pending.append(copy)
        return copy

    def halves(t, at, h, last=False):
        start, size = (at % sections) * piece + h * part, part
        if last:
            start, size = start + h * cut, part - cut
        align = cut if cut else part
        return proj.at[t, pl.ds(pl.multiple_of(start, align), size)]

    def line_ref(t, h):
        if h < 2:
            return halves(t, place, h)
        start = (place + half_ring) % sections * piece + part - cut
        return proj.at[t, pl.ds(pl.multiple_of(start, cut), 2 * cut)]

    own_copy.wait()

    def line_copy(source, h, step):
        ref = line_ref(source * 2 + core, h)
        return pltpu.make_async_remote_copy(
            src_ref=ref, dst_ref=ref,
            send_sem=line_s.at[source, h, (step + 1) // 2], recv_sem=line_r.at[source, h],
            device_id={"tok": (chip + step + chips) % chips * 2 + core},
            device_id_type=pl.DeviceIdType.MESH,
        )

    def along(source, h, action):
        for step in (-1, 1):
            inside = chip + step <= chips - 1 if step == 1 else chip + step >= 0
            away = source <= chip if step == 1 else source >= chip

            @pl.when(jnp.logical_and(inside, away))
            def _():
                action(line_copy(source, h, step))

    for h in range(2):
        along(chip, h, lambda copy: copy.start())
    outer_chip = jnp.minimum(chip, chips - 1 - chip) == 0
    if cut:
        @pl.when(outer_chip)
        def _():
            along(chip, 2, lambda copy: copy.start())
    partner_slab = send(proj.at[tok], proj.at[tok], d2d_own.at[0], d2d_own.at[1], tok=partner)

    def multiply(n, first=False):
        loads[n].wait()
        product = jnp.dot(acts[n], proj[order[n]], preferred_element_type=F32)
        if first:
            total[...] = product
        else:
            total[...] += product

    multiply(0, True)
    partner_slab.wait_recv()
    multiply(1)

    def multiply_piece(n, at):
        rows_of = pl.ds(pl.multiple_of(at % sections * piece, piece), piece)
        total[...] += jnp.dot(
            acts[n, :, rows_of], proj[order[n], rows_of], preferred_element_type=F32
        )

    split_last = piece % 128 == 0
    shared = {k: [] for k in range(1, chips)}
    late = {k: [] for k in range(1, chips)}
    ring = {}

    def share(k, ref, opposite=False):
        n = len(shared[k]) + len(late[k])
        copy = send(ref, ref, d2d_s.at[k - 1, n], d2d_r.at[k - 1, n], tok=partner)
        (late if opposite else shared)[k].append(copy)

    def pass_on(k, j, way, h, ref):
        ring[k, j, way, h] = send(
            ref, ref, ring_s.at[k - 1, j - 1, way, h], ring_r.at[k - 1, j - 1, way, h],
            section=(to_right if way == 0 else to_left),
        )

    events = []
    for k in range(1, chips):
        events.append((0.75 * k + 0.2, k, 0))
        for j in range(1, half_ring + 1):
            events.append((1.5 * k + 1.4 * j - 1.1, k, j))
        if cut:
            events.append((0.75 * chips - 0.5 if k == 1 else 3.3 + 0.02 * k, k, -1))
        if k == chips - 1 and split_last:
            events.append((1.5 * k + 1.4 * half_ring - 1.15, k, half_ring + 1))
            events.append((1.5 * k + 1.4 * half_ring - 0.9, k, half_ring + 2))
        else:
            events.append((1.5 * k + 1.4 * half_ring - 0.9, k, half_ring + 1))
    for _, k, j in sorted(events):
        t = order[2 * k]
        source = t // 2
        if j < 0:
            line_copy(source, 2, 1).wait_recv()
            along(source, 2, lambda copy: copy.start())
            share(k, line_ref(t, 2), True)
        elif j == 0:
            for h in range(2):
                line_copy(source, h, 1).wait_recv()
                ref = halves(t, place, h)
                along(source, h, lambda copy: copy.start())
                for way in range(2):
                    if half_ring > 1 or way == h:
                        pass_on(k, 1, way, h, halves(t, place, h, half_ring == 1))
                share(k, ref)
            if k == min(2, chips - 1) and cut:
                @pl.when(jnp.logical_not(outer_chip))
                def _():
                    along(chip, 2, lambda copy: copy.start())
        elif j <= half_ring:
            for h in range(2):
                for way in range(2):
                    if j == half_ring and way != h:
                        continue
                    ring[k, j, way, h].wait_recv()
                    at = place + sections - j if way == 0 else place + j
                    if j < half_ring and (j + 1 < half_ring or way == h):
                        pass_on(k, j + 1, way, h, halves(t, at, h, j + 1 == half_ring))
                    share(k, halves(t, at, h, j == half_ring), j == half_ring)
        elif k == chips - 1 and split_last:
            if j == half_ring + 1:
                near = [place]
                for step in range(1, half_ring):
                    near += [place + step, place + sections - step]
                loads[2 * k].wait()
                for at in near:
                    multiply_piece(2 * k, at)
                for copy in shared[k]:
                    copy.wait_recv()
                loads[2 * k + 1].wait()
                for at in near:
                    multiply_piece(2 * k + 1, at)
            else:
                multiply_piece(2 * k, place + half_ring)
                for copy in late[k]:
                    copy.wait_recv()
                multiply_piece(2 * k + 1, place + half_ring)
        else:
            multiply(2 * k)
            for copy in shared[k] + late[k]:
                copy.wait_recv()
            multiply(2 * k + 1)

    mean_out[...] = jnp.zeros_like(mean_out)
    for l in range(layers):
        block = total[l * tok_rows : (l + 1) * tok_rows]
        mean = jnp.sum(block, axis=0, keepdims=True) / tok_rows
        mean_out[l : l + 1] = mean
        block = block - mean
        high = block.astype(BF16)
        low = (block - high.astype(F32)).astype(BF16)
        left_op[l, :tok_rows] = high
        left_op[l, tok_rows : 2 * tok_rows] = high
        left_op[l, 2 * tok_rows :] = low
        right_op[l, :tok_rows] = high
        right_op[l, tok_rows : 2 * tok_rows] = low
        right_op[l, 2 * tok_rows :] = high
    mean_copies = []
    for k in range(1, groups):
        mean_copies.append(
            send(mean_out, means.at[k - 1], mean_s.at[k - 1], mean_r.at[k - 1], tok=flip(tok, k, groups))
        )

    low_side = chip < chips // 2
    rank = jnp.where(low_side, chip, chips - 1 - chip)

    def mirror(d):
        return jnp.where(low_side, d, chips - 1 - d)

    pair = {}
    outward = [chips - 1 - d for d in range(chips)]
    for l in range(layers):
        product = lax.dot_general(
            left_op[l], right_op[l], (((0,), (0,)), ((), ())), preferred_element_type=F32
        )
        for t in range(groups):
            gram[t, l] = product[t * slab : (t + 1) * slab]
        for d in outward:
            pair[d, l] = send(
                gram.at[mirror(d) * 2 + 1 - core, l], pair_in.at[d, l], pair_s.at[d, l], pair_r.at[d, l],
                tok=partner,
            )

    def line_sum(d, l, primary):
        upward = low_side if primary else jnp.logical_not(low_side)
        way = jnp.where(upward, 0, 1)
        target = mirror(d)
        return pltpu.make_async_remote_copy(
            src_ref=gram.at[target * 2 + core, l], dst_ref=line_in.at[way, target, l],
            send_sem=gl_s.at[way, target, l], recv_sem=gl_r.at[way, target, l],
            device_id={"tok": jnp.clip(jnp.where(upward, chip + 1, chip - 1), 0, chips - 1) * 2 + core},
            device_id_type=pl.DeviceIdType.MESH,
        )

    def add_pair(d, l):
        pair[d, l].wait_recv()
        mine = mirror(d) * 2 + core
        gram[mine, l] = gram[mine, l] + pair_in[d, l]

    def arrive(d, l, primary):
        upward = low_side if primary else jnp.logical_not(low_side)
        way = jnp.where(upward, 0, 1)
        target = mirror(d)
        line_sum(d, l, primary).wait_recv()
        mine = target * 2 + core
        gram[mine, l] = gram[mine, l] + line_in[way, target, l]

    def arrive_own(l, primary):
        upward = low_side if primary else jnp.logical_not(low_side)
        way = jnp.where(upward, 0, 1)
        pltpu.make_async_remote_copy(
            src_ref=gram.at[tok, l], dst_ref=line_in.at[way, chip, l],
            send_sem=gl_s.at[way, chip, l], recv_sem=gl_r.at[way, chip, l],
            device_id={"tok": partner}, device_id_type=pl.DeviceIdType.MESH,
        ).wait_recv()
        gram[tok, l] = gram[tok, l] + line_in[way, chip, l]

    def forward(d, l, primary):
        @pl.when(d > rank if primary else d < rank)
        def _():
            if primary:
                @pl.when(rank > 0)
                def _():
                    arrive(d, l, primary)
            else:
                arrive(d, l, primary)
            line_sum(d, l, primary).start()

    def correct():
        for copy in mean_copies:
            copy.wait_recv()
        overall = mean_out[...]
        for k in range(1, groups):
            overall = overall + means[k - 1]
        overall = overall / groups
        for l in range(layers):
            shifts = [mean_out[l : l + 1] - overall[l : l + 1]]
            for k in range(1, groups):
                shifts.append(means[k - 1, l : l + 1] - overall[l : l + 1])
            shifts = jnp.concatenate(shifts, axis=0)
            outer = lax.dot_general(
                shifts, shifts * tok_rows, (((0,), (0,)), ((), ())),
                precision=lax.Precision.HIGHEST, preferred_element_type=F32,
            )
            for t in range(groups):
                corr[t, l] = outer[t * slab : (t + 1) * slab]

    steps = []
    for d in range(chips):
        for l in range(layers):
            turn = (chips - 1 - d) * layers + l
            steps.append((turn, 1, d, l))
            if d < chips - 1:
                steps.append((d * layers + l + layers - 0.5, 0, d, l))
    early = True
    for turn, primary, d, l in sorted(steps):
        if turn > layers - 1 and early:
            early = False
            for other in outward[1:]:
                for m in range(layers):
                    add_pair(other, m)
            correct()
        if early:
            add_pair(d, l)
        if d > 0 or not primary:
            forward(d, l, bool(primary))

    edge = None
    for l in range(layers):
        @pl.when(rank > 0)
        def _():
            arrive_own(l, True)

        arrive_own(l, False)
        result = gram[tok, l] + corr[tok, l]
        sketch_ref[l] = result
        if l == 0:
            edge_out[...] = result.astype(BF16)
            edge = send(
                edge_out, edge_in, edge_s, edge_r, section=(section + sections - 1) % sections
            )

    def inner(first, second):
        columns = jnp.sum(first * second, axis=0, keepdims=True)
        lanes = columns[:, :128]
        for start in range(128, width, 128):
            lanes = lanes + columns[:, start : start + 128]
        return lanes

    prod_out[...] = jnp.zeros_like(prod_out)
    own = [sketch_ref[l] for l in range(layers)]
    for l in range(layers):
        prod_out[l : l + 1] = inner(own[l], own[l])
        if l:
            prod_out[layers + l - 1 : layers + l] = inner(own[l - 1], own[l])
    base = 2 * layers - 1
    edge.wait_recv()
    beyond = edge_in[...].astype(F32)
    prod_out[base : base + 1] = inner(own[-1], beyond)
    prod_out[base + 1 : base + 2] = inner(beyond, beyond)
    prod_copies, prev_copies = [], []
    for k in range(groups):
        other = flip(tok, k, groups)
        prev_copies.append(
            send(prod_out, prev_prods.at[k], prev_s.at[k], prev_r.at[k],
                 section=(section + 1) % sections, tok=other)
        )
        if k:
            prod_copies.append(
                send(prod_out, prods.at[k - 1], prod_s.at[k - 1], prod_r.at[k - 1], tok=other)
            )
    products = prod_out[...]
    for k in range(1, groups):
        prod_copies[k - 1].wait_recv()
        products = products + prods[k - 1]
    prev_copies[0].wait_recv()
    earlier = prev_prods[0]
    for k in range(1, groups):
        prev_copies[k].wait_recv()
        earlier = earlier + prev_prods[k]
    products = jnp.broadcast_to(jnp.sum(products, axis=1, keepdims=True), products.shape)
    earlier = jnp.broadcast_to(jnp.sum(earlier, axis=1, keepdims=True), earlier.shape)

    def item(i):
        return products[i : i + 1]

    first, last = section == 0, section == sections - 1
    before = jnp.where(first, item(0), earlier[layers - 1 : layers])
    before_cross = jnp.where(first, item(0), earlier[base : base + 1])
    beyond_square = jnp.where(last, item(layers - 1), item(base + 1))
    beyond_cross = jnp.where(last, item(layers - 1), item(base))
    squares = [before] + [item(l) for l in range(layers)] + [beyond_square]
    chained = [before_cross] + [item(layers + l) for l in range(layers - 1)] + [beyond_cross]
    ratios = [chained[i] / jnp.sqrt(squares[i] * squares[i + 1]) for i in range(layers + 1)]
    sim_ref[...] = jnp.zeros_like(sim_ref)
    lane = lax.broadcasted_iota(jnp.int32, (1, 128), 1)
    for l in range(layers):
        sim_ref[l : l + 1] = jnp.where(lane == 0, ratios[l], ratios[l + 1])

    for copy in pending:
        copy.wait_send()
    for d in range(chips):
        for l in range(layers):
            for primary in (True, False):
                @pl.when(d > rank if primary else d < rank)
                def _():
                    line_sum(d, l, primary).wait_send()
    for source in [chip] + [t // 2 for t in order[2::2]]:
        for h in range(3 if cut else 2):
            along(source, h, lambda copy: copy.wait_send())


def finish(sketch_in, sim_in, sketch_out, sim_out):
    sketch_out[...] = sketch_in[...]
    sim_out[...] = sim_in[: sim_out.shape[0], : sim_out.shape[1]]


def local(sections, groups, activations, projection):
    layers, tok_rows, model_width = activations.shape
    depth, width = projection.shape
    rows = layers * tok_rows
    chips, slab = groups // 2, width // groups
    tall = -(-(2 * layers + 3) // 8) * 8
    dma = pltpu.SemaphoreType.DMA
    sketch, sim = pl.pallas_call(
        functools.partial(kernel, sections, groups, layers),
        out_shape=(
            jax.ShapeDtypeStruct((layers, slab, width), F32),
            jax.ShapeDtypeStruct((tall, 128), F32),
        ),
        in_specs=[pl.BlockSpec(memory_space=pl.ANY)] * 2,
        out_specs=(pl.BlockSpec(memory_space=pltpu.VMEM),) * 2,
        scratch_shapes=[
            pltpu.VMEM((groups, rows, depth), BF16),
            pltpu.VMEM((groups, depth, width), BF16),
            pltpu.VMEM((rows, width), F32),
            pltpu.VMEM((layers, 3 * tok_rows, width), BF16),
            pltpu.VMEM((layers, 3 * tok_rows, width), BF16),
            pltpu.VMEM((groups, layers, slab, width), F32),
            pltpu.VMEM((chips, layers, slab, width), F32),
            pltpu.VMEM((2, chips, layers, slab, width), F32),
            pltpu.VMEM((tall, width), F32),
            pltpu.VMEM((groups - 1, tall, width), F32),
            pltpu.VMEM((groups, layers, slab, width), F32),
            pltpu.VMEM((slab, width), BF16),
            pltpu.VMEM((slab, width), BF16),
            pltpu.VMEM((tall, 128), F32),
            pltpu.VMEM((groups - 1, tall, 128), F32),
            pltpu.VMEM((groups, tall, 128), F32),
            dma((groups,)), dma(()), dma((2,)),
            dma((chips, 3, 2)), dma((chips, 3)),
            dma((chips - 1, sections // 2, 2, 2)), dma((chips - 1, sections // 2, 2, 2)),
            dma((chips - 1, 2 * sections + 1)), dma((chips - 1, 2 * sections + 1)),
            dma((groups - 1,)), dma((groups - 1,)),
            dma((chips, layers)), dma((chips, layers)),
            dma((2, chips, layers)), dma((2, chips, layers)),
            dma(()), dma(()),
            dma((groups - 1,)), dma((groups - 1,)),
            dma((groups,)), dma((groups,)),
        ],
        compiler_params=pltpu.CompilerParams(
            collective_id=0, has_side_effects=True, vmem_limit_bytes=60 * 1024 * 1024
        ),
    )(activations.reshape(rows, model_width), projection)
    sketch, similarity = pl.pallas_call(
        finish,
        out_shape=(
            jax.ShapeDtypeStruct((layers, slab, width), F32),
            jax.ShapeDtypeStruct((layers, 2), F32),
        ),
        in_specs=[pl.BlockSpec(memory_space=pltpu.VMEM)] * 2,
        out_specs=(pl.BlockSpec(memory_space=pltpu.VMEM),) * 2,
    )(sketch, sim)
    return jnp.swapaxes(sketch, 1, 2), similarity


def solution(mesh):
    return jax.shard_map(
        functools.partial(local, mesh.shape["section"], mesh.shape["tok"]),
        mesh=mesh,
        in_specs=(P("section", "tok", None), P("tok", None)),
        out_specs=(P("section", None, "tok"), P("section", None)),
        check_vma=False,
    )
```
